32 devices in a mesh: dp: 2 (over core), row: 4 (over y, x), col: 4 (over z).
Axes of the slice: x: 2, y: 2, z: 4, core: 2. Of those that a mesh axis runs over, the one named last changes fastest.
Arguments:
- states: bfloat16 [3072, 4096], P(('dp', 'row'), 'col'), may hold values from -6 to 6
- actions: bfloat16 [3072, 24], P(('dp', 'row')), may hold values from -6 to 6
- rewards: float32 [3072], P(('dp', 'row')), may hold values from -6 to 6
- terminal: int32 [3072], P(('dp', 'row')), may hold values 0 or 1
- next_index: int32 [3072], P(('dp', 'row')), may hold values from 0 to 3071
- hidden_weights: bfloat16 [4, 4096, 4096], P(None, 'col', 'row'), may hold values from -0.09375 to 0.09375
- action_weights: bfloat16 [2, 24, 4096], replicated, may hold values from -1.25 to 1.25
- heads: bfloat16 [4096, 27], replicated, may hold values from -0.09375 to 0.09375
- policy_scale: float32 [24], replicated, may hold values from 0.5 to 2
Outputs:
- advantage: float32 [3072], P(('dp', 'row'))
- losses: float32 [3], replicated
- head_grads: float32 [4096, 27], replicated
The draws below stay inside these ranges and needn't reach their ends.
Inputs may be any that keep to these rules, and one draw needn't show every extreme that they name: `next_index`: any batch row, from any device.
All inputs are finite; a program needn't handle non-finite values. No bound on the sum of `terminal` on one device may be relied on, other than what follows from the above.
Results may differ from the reference program's by a relative error of at most 0.0038.
Values may be sent and summed in bfloat16 or wider, within the bound.
No kernel may reach another device: no remote copies, remote signals or barrier semaphores. Data moves between devices by JAX's collectives and lax.ppermute only.
A program may use at most 128 MiB of HBM per device.

```python
import math
import jax
import jax.numpy as jnp
from jax import lax

D = 4096
ACT = 24
TOKENS = 3072


def with_ends(result, rng, smallest, high):
    place = [jax.random.randint(jax.random.fold_in(rng, axis), (), 0, length) for axis, length in enumerate(result.shape)]
    longest = result.shape.index(max(result.shape))
    beside = place[:longest] + [(place[longest] + 1) % result.shape[longest]] + place[longest + 1:]
    return result.at[tuple(place)].set(smallest).at[tuple(beside)].set(high)


def steps_of(rng, shape, shards, low, top_value):
    def one(dim, blocks):
        draws = jax.random.uniform(jax.random.fold_in(jax.random.fold_in(rng, 6), dim), (blocks,), jnp.float32, low / len(shards), top_value / len(shards))
        return jnp.repeat(jnp.exp(draws), shape[dim] // blocks).reshape((-1,) + (1,) * (len(shape) - dim - 1))

    factor_of = one(*shards[0])
    for cut in shards[1:]:
        factor_of = factor_of * one(*cut)
    return factor_of


def gaussian(own_key, extent, scale, reach, split=(), held_as=jnp.bfloat16):
    values = jax.random.normal(own_key, extent, jnp.float32) * scale
    if len(split) > 0:
        values = steps_of(own_key, extent, split, -0.22, 0.18) * values
    return jnp.clip(values, min=-reach, max=reach).astype(held_as)


def setup_inputs(seed: int = 0) -> dict:
    seeds = jax.random.split(jax.random.key(seed), 10)
    states = gaussian(seeds[0], (TOKENS, D), 1.0, 6.0, ((0, 8), (1, 4)))
    actions = gaussian(seeds[1], (TOKENS, ACT), 1.0, 6.0, ((0, 8),))
    rewards = gaussian(seeds[2], (TOKENS,), 1.0, 6.0, ((0, 8),), jnp.float32)
    terminal = with_ends((jax.random.randint(seeds[3], (TOKENS,), 0, 8) < 1).astype(jnp.int32), jax.random.fold_in(seeds[3], 1), 0, 1)
    next_index = with_ends(jax.random.randint(seeds[4], (TOKENS,), 0, TOKENS), jax.random.fold_in(seeds[4], 1), 0, TOKENS - 1).astype(jnp.int32)
    hidden_weights = gaussian(seeds[5], (4, D, D), D ** -0.5, 0.09375, ((1, 4), (2, 4)))
    action_weights = gaussian(seeds[6], (2, ACT, D), ACT ** -0.5, 1.25)
    heads = gaussian(seeds[7], (D, 3 + ACT), D ** -0.5, 0.09375)
    policy_scale = jnp.clip(jnp.exp(jax.random.uniform(seeds[8], (ACT,), jnp.float32, math.log(0.5), math.log(2.0))), 0.5, 2.0)
    return {"states": states, "actions": actions, "rewards": rewards, "terminal": terminal, "next_index": next_index, "hidden_weights": hidden_weights, "action_weights": action_weights, "heads": heads, "policy_scale": policy_scale}


GAMMA = 0.99
TAU = 0.7
FLOOR = 0.01

def reference(states, actions, rewards, terminal, next_index, hidden_weights, action_weights, heads, policy_scale):
    hidden = []
    for network in range(4):
        pre = jnp.dot(states, hidden_weights[network], preferred_element_type=jnp.float32)
        if network < 2:
            pre = pre + jnp.dot(actions, action_weights[network], preferred_element_type=jnp.float32)
        hidden.append(jnp.maximum(pre, 0.0).astype(jnp.bfloat16))
    first_q = jnp.dot(hidden[0], heads[:, 0], preferred_element_type=jnp.float32)
    second_q = jnp.dot(hidden[1], heads[:, 1], preferred_element_type=jnp.float32)
    value = jnp.dot(hidden[2], heads[:, 2], preferred_element_type=jnp.float32)
    policy_mean = jnp.dot(hidden[3], heads[:, 3:], preferred_element_type=jnp.float32)
    advantage = jnp.minimum(first_q, second_q) - value
    target = rewards + GAMMA * (1.0 - terminal.astype(jnp.float32)) * value[next_index.astype(jnp.int32)]
    top = jnp.max(advantage)
    weight = jnp.maximum(jnp.exp(advantage - top), FLOOR)
    expectile = jnp.where(advantage >= 0.0, TAU, 1.0 - TAU)
    scaled = (actions.astype(jnp.float32) - policy_mean) / policy_scale
    log_prob = -0.5 * lax.optimization_barrier(jnp.sum(scaled * scaled, axis=1))
    losses = jnp.stack([jnp.sum(expectile * advantage * advantage), jnp.sum((first_q - target) ** 2 + (second_q - target) ** 2), -jnp.sum(weight * log_prob)]) / TOKENS
    coeff_policy = -weight[:, None] * scaled / policy_scale
    columns = [(hidden[0], (2.0 * (first_q - target))[:, None]), (hidden[1], (2.0 * (second_q - target))[:, None]), (hidden[2], (-2.0 * expectile * advantage)[:, None]), (hidden[3], coeff_policy)]
    grads = jnp.concatenate([jnp.dot(units.astype(jnp.float32).T, coeff, precision=lax.Precision.HIGHEST) for units, coeff in columns], axis=1)
    return (advantage, losses, grads / jnp.sqrt(jnp.float32(TOKENS)))
```

```python
import functools
import math

import jax
import jax.numpy as jnp
from jax import lax
from jax.experimental import pallas as pl
from jax.experimental.pallas import tpu as pltpu
from jax.sharding import PartitionSpec as P


GAMMA = 0.99
TAU = 0.7
FLOOR = 0.01
ORDER = (3, 2, 0, 1)
F32 = jnp.float32
BF16 = jnp.bfloat16


def swap(x, axis, bit):
    size = lax.axis_size(axis)
    return lax.ppermute(x, axis, [(i, i ^ bit) for i in range(size)])


def spread(x, axes):
    size = math.prod(lax.axis_size(a) for a in axes)
    x = jnp.broadcast_to(x[None], (size,) + x.shape)
    return lax.all_to_all(x, axes, 0, 0, tiled=True)


def bits_of(size):
    return [1 << b for b in range(size.bit_length() - 1)]


def net_kernel(row_ref, *refs, places, row_count, nets, with_actions):
    count = len(places)
    pieces = refs[:count]
    own_ref, other_ref = refs[count : count + 2]
    at = count + 2
    head_refs = refs[at : at + nets]
    at += nets
    if with_actions:
        act_ref, act_w_ref = refs[at : at + 2]
        at += 2
    hidden_refs = refs[at : at + nets]
    part_refs = refs[at + nets : at + 2 * nets]
    buf, w_buf, sems, w_sems = refs[at + 2 * nets :]
    w_copies = [
        pltpu.make_async_copy(ref, w_buf.at[i], w_sems.at[i])
        for i, ref in enumerate((own_ref, other_ref))
    ]
    copies = [
        pltpu.make_async_copy(pieces[i], buf.at[j, :, pl.ds(start, size), :], sems.at[i])
        for i, (j, start, size) in enumerate(places)
    ]
    row = row_ref[0]
    w_copies[0].start()
    for j in range(row_count):
        for i, (jj, _, _) in enumerate(places):
            if jj == j:
                copies[i].start()
        if j == 0:
            w_copies[1].start()
    for w_copy in w_copies:
        w_copy.wait()
    for j in range(row_count):
        for i, (jj, _, _) in enumerate(places):
            if jj == j:
                copies[i].wait()
        where = jnp.bitwise_xor(row, j)
        for n in range(nets):
            acc = jnp.dot(buf[j, 0], w_buf[0, n], preferred_element_type=F32)
            acc = acc + jnp.dot(buf[j, 1], w_buf[1, n], preferred_element_type=F32)
            if with_actions:
                acc = acc + jnp.dot(act_ref[where], act_w_ref[n], preferred_element_type=F32)
            hidden = jnp.maximum(acc, 0.0).astype(BF16)
            hidden_refs[n][where] = hidden
    for n in range(nets):
        for j in range(row_count):
            part_refs[n][j] = lax.dot_general(
                head_refs[n][...], hidden_refs[n][j], (((1,), (1,)), ((), ())),
                preferred_element_type=F32,
            )


def run_nets(row_at, pieces, places, w_own, w_other, heads, rows, row_count, extra):
    nets, depth, units = w_own.shape
    any_spec = pl.BlockSpec(memory_space=pl.ANY)
    vmem = pl.BlockSpec(memory_space=pltpu.VMEM)
    smem = pl.BlockSpec(memory_space=pltpu.SMEM)
    late = [w_own, w_other, *heads, *extra]
    tokens = row_count * rows
    wide = max(units, 128)
    held = 4 * tokens * depth + 8 * nets * depth * wide + 4 * nets * tokens * wide
    outs = pl.pallas_call(
        functools.partial(
            net_kernel, places=places, row_count=row_count, nets=nets,
            with_actions=bool(extra),
        ),
        out_shape=tuple(
            [jax.ShapeDtypeStruct((row_count, rows, units), BF16)] * nets
            + [jax.ShapeDtypeStruct((row_count, h.shape[0], rows), F32) for h in heads]
        ),
        in_specs=[smem] + [any_spec] * (len(pieces) + 2) + [vmem] * (len(late) - 2),
        out_specs=tuple([vmem] * (2 * nets)),
        scratch_shapes=[
            pltpu.VMEM((row_count, 2, rows, depth), BF16),
            pltpu.VMEM((2, nets, depth, units), BF16),
            pltpu.SemaphoreType.DMA((len(pieces),)),
            pltpu.SemaphoreType.DMA((2,)),
        ],
        compiler_params=pltpu.CompilerParams(vmem_limit_bytes=held + 4 * 1024 * 1024),
        cost_estimate=pl.CostEstimate(
            flops=4 * nets * tokens * depth * units,
            bytes_accessed=4 * tokens * depth,
            transcendentals=0,
        ),
    )(row_at.reshape(1), *pieces, *late)
    return outs[:nets], outs[nets:]


def split_dot(coeff, hidden):
    high = coeff.astype(BF16)
    low = (coeff - high.astype(F32)).astype(BF16)
    out = jnp.dot(high, hidden, preferred_element_type=F32)
    return out + jnp.dot(low, hidden, preferred_element_type=F32)


def tail_kernel(
    dp_ref, late_ref, pack_ref, known_ref, scale_ref, h0, h1, h2, h3,
    adv_ref, out_ref, grad_ref, *, acts,
):
    tokens = late_ref.shape[-1]
    dp = dp_ref[0]
    values = [known_ref[acts + d : acts + d + 1] for d in range(2)]
    advs = [
        jnp.minimum(late_ref[2 * d : 2 * d + 1], late_ref[2 * d + 1 : 2 * d + 2]) - values[d]
        for d in range(2)
    ]
    first, second, adv = late_ref[0:1], late_ref[1:2], advs[0]
    top = functools.reduce(jnp.maximum, [jnp.max(a) for a in advs])
    values = [jnp.where(dp == 0, values[0], values[1]), jnp.where(dp == 0, values[1], values[0])]
    rewards = pack_ref[acts : acts + 1]
    terminal = pack_ref[acts + 1 : acts + 2]
    index = pack_ref[acts + 2 : acts + 3].astype(jnp.int32)
    lanes = 128
    groups = tokens // lanes
    table = jnp.concatenate(
        [v[:, g * lanes : (g + 1) * lanes] for v in values for g in range(groups)], axis=0
    )
    high = jnp.right_shift(index, 7)
    low = jnp.bitwise_and(index, lanes - 1)
    pick_high = (lax.broadcasted_iota(jnp.int32, (table.shape[0], tokens), 0) == high).astype(F32)
    rows = lax.dot_general(
        table, pick_high, (((0,), (0,)), ((), ())), precision=lax.Precision.HIGHEST,
        preferred_element_type=F32,
    )
    pick_low = lax.broadcasted_iota(jnp.int32, (lanes, tokens), 0) == low
    following = jnp.sum(jnp.where(pick_low, rows, 0.0), axis=0, keepdims=True)
    target = rewards + GAMMA * (1.0 - terminal) * following
    weight = jnp.maximum(jnp.exp(adv - top), FLOOR)
    expectile = jnp.where(adv >= 0.0, TAU, 1.0 - TAU)
    scale = scale_ref[...]
    scaled = (pack_ref[0:acts] - known_ref[0:acts]) / scale
    log_prob = -0.5 * jnp.sum(scaled * scaled, axis=0, keepdims=True)
    gap0 = first - target
    gap1 = second - target
    loss0 = jnp.sum(expectile * adv * adv)
    loss1 = jnp.sum(gap0 * gap0 + gap1 * gap1)
    loss2 = -jnp.sum(weight * log_prob)
    adv_ref[...] = adv
    lane = lax.broadcasted_iota(jnp.int32, (1, grad_ref.shape[1]), 1)
    loss = jnp.where(lane == 0, loss0, jnp.where(lane == 1, loss1, jnp.where(lane == 2, loss2, 0.0)))
    high = loss.astype(BF16).astype(F32)
    grad_ref[acts + 3 : acts + 4] = high
    grad_ref[acts + 4 : acts + 5] = loss - high
    grad_ref[0:1] = split_dot(2.0 * gap0, h0[...])
    grad_ref[1:2] = split_dot(2.0 * gap1, h1[...])
    grad_ref[2:3] = split_dot(-2.0 * expectile * adv, h2[...])
    grad_ref[3 : 3 + acts] = split_dot(-weight * scaled / scale, h3[...])
    out = grad_ref[...].astype(BF16)
    for i in range(out_ref.shape[0]):
        out_ref[i] = out


def shards(
    states, actions, rewards, terminal, next_index, hidden_weights, action_weights, heads, policy_scale
):
    rows, feats = states.shape
    acts = actions.shape[1]
    nets, _, row_units = hidden_weights.shape
    row_count = lax.axis_size("row")
    col_count = lax.axis_size("col")
    dp_count = lax.axis_size("dp")
    dp_at = lax.axis_index("dp")
    row_at = lax.axis_index("row")
    col_at = lax.axis_index("col")
    peers = row_count * col_count
    units = row_units // col_count
    half = feats // 2
    tokens = rows * row_count
    total = tokens * dp_count
    shares = (1, 2, 3, 3, 3) if rows % 192 == 0 else (1,)
    sizes = [rows * s // sum(shares) for s in shares]
    starts = [sum(sizes[:c]) for c in range(len(sizes))]

    pack = jnp.concatenate(
        [
            actions.astype(F32).T,
            rewards[None],
            terminal.astype(F32)[None],
            next_index.astype(F32)[None],
        ],
        axis=0,
    )
    pack = spread(pack, ("row",))
    own_actions = pack[:, :acts].transpose(0, 2, 1).astype(BF16)
    pack = pack.transpose(1, 0, 2).reshape(acts + 3, tokens)

    col_bits = bits_of(col_count)[::-1]
    cols = [0]
    for bit in col_bits:
        cols = cols + [c ^ bit for c in cols]
    pair = states.reshape(rows, 2, half).transpose(1, 0, 2)
    pair = jnp.where(dp_at == 0, pair, pair[::-1])
    pieces, places = [], []
    for c, (start, size) in enumerate(zip(starts, sizes)):
        block = pair[:, start : start + size]
        for bit in col_bits:
            block = jnp.concatenate([block, swap(block, "col", bit)], axis=2)
        held = {0: block}
        order = bits_of(row_count)
        if c % 2:
            order = order[::-1]
        for bit in order:
            for j, value in list(held.items()):
                held[j ^ bit] = swap(value, "row", bit)
        for j in range(row_count):
            pieces.append(held[j])
            places.append((j, start, size))

    hidden, parts = {}, {}
    unit_at = row_at * row_units + col_at * units
    heads_t = lax.dynamic_slice_in_dim(heads.T, unit_at, units, 1)
    act_w = lax.dynamic_slice_in_dim(action_weights, unit_at, units, 2)
    for first in range(0, nets, 2):
        group = ORDER[first : first + 2]
        low = min(group)
        mine = lax.dynamic_slice(
            hidden_weights, (low, dp_at * half, 0), (len(group), half, row_units)
        )
        got = []
        for k in cols:
            sent = lax.dynamic_slice_in_dim(mine, jnp.bitwise_xor(col_at, k) * units, units, 2)
            got.append(swap(sent, "col", k) if k else sent)
        w_own = jnp.concatenate(got, axis=1)
        w_other = swap(w_own, "dp", 1)
        group = range(low, low + len(group))
        head = [
            heads_t[3:] if n == 3 else jnp.pad(heads_t[n : n + 1], ((0, 7), (0, 0))) for n in group
        ]
        extra = (own_actions, act_w) if low == 0 else ()
        got_hidden, got_parts = run_nets(
            row_at, pieces, places, w_own, w_other, head, rows, row_count, extra
        )
        for i, n in enumerate(group):
            hidden[n], parts[n] = got_hidden[i].reshape(tokens, units), got_parts[i]

    piece = tokens // peers
    known = jnp.concatenate([parts[3], parts[2][:, :1]], axis=1)
    known = known.transpose(1, 0, 2).reshape(acts + 1, peers, piece).transpose(1, 0, 2)
    known = lax.all_to_all(known, ("row", "col"), 0, 0, tiled=True)
    known = jnp.sum(known, axis=0)
    known = jnp.concatenate([known, swap(known[acts:], "dp", 1)], axis=0)
    known = spread(known, ("row", "col"))
    known = known.transpose(1, 0, 2).reshape(acts + 2, tokens)

    late = jnp.concatenate([parts[n][:, 0].reshape(1, tokens) for n in (0, 1)], axis=0)
    for axis, size in (("col", col_count), ("row", row_count)):
        late = sum((swap(late, axis, k) for k in range(1, size)), late)
    late = jnp.concatenate([late, swap(late, "dp", 1)], axis=0)

    vmem = pl.BlockSpec(memory_space=pltpu.VMEM)
    smem = pl.BlockSpec(memory_space=pltpu.SMEM)
    adv, last = pl.pallas_call(
        functools.partial(tail_kernel, acts=acts),
        out_shape=(
            jax.ShapeDtypeStruct((1, tokens), F32),
            jax.ShapeDtypeStruct((dp_count * peers, acts + 5, units), BF16),
        ),
        in_specs=[smem] + [vmem] * 8,
        out_specs=(vmem, vmem),
        scratch_shapes=[pltpu.VMEM((acts + 5, units), F32)],
        compiler_params=pltpu.CompilerParams(vmem_limit_bytes=24 * 1024 * 1024),
    )(
        dp_at.reshape(1), late, pack, known, policy_scale[:, None],
        hidden[0], hidden[1], hidden[2], hidden[3],
    )
    advantage = lax.dynamic_slice_in_dim(adv[0], row_at * rows, rows, 0)
    last = lax.all_to_all(last, ("dp", "row", "col"), 0, 0, tiled=True)
    last = last.reshape(dp_count, peers, acts + 5, units)
    summed = jnp.sum(last.astype(F32), axis=0)
    grads = summed[:, : acts + 3].transpose(1, 0, 2).reshape(acts + 3, peers * units)
    grads = (grads / math.sqrt(total)).T
    losses = (summed[0, acts + 3, :3] + summed[0, acts + 4, :3]) / total
    return advantage, losses, grads


def solution(mesh):
    return jax.shard_map(
        shards,
        mesh=mesh,
        in_specs=(
            P(("dp", "row"), "col"),
            P(("dp", "row"), None),
            P(("dp", "row")),
            P(("dp", "row")),
            P(("dp", "row")),
            P(None, "col", "row"),
            P(),
            P(),
            P(),
        ),
        out_specs=(P(("dp", "row")), P(), P()),
        check_vma=False,
    )
```

```python
import functools
import math

import jax
import jax.numpy as jnp
from jax import lax
from jax.experimental import pallas as pl
from jax.experimental.pallas import tpu as pltpu
from jax.sharding import PartitionSpec as P


GAMMA = 0.99
TAU = 0.7
FLOOR = 0.01
F32 = jnp.float32
BF16 = jnp.bfloat16


def swap(x, axis, bit):
    size = lax.axis_size(axis)
    return lax.ppermute(x, axis, [(i, i ^ bit) for i in range(size)])


def spread(x, axes):
    size = math.prod(lax.axis_size(a) for a in axes)
    x = jnp.broadcast_to(x[None], (size,) + x.shape)
    return lax.all_to_all(x, axes, 0, 0, tiled=True)


def bits_of(size):
    return [1 << b for b in range(size.bit_length() - 1)]


def net_kernel(row_ref, *refs, places, row_count, picks, with_actions):
    nets = len(picks)
    count = len(places)
    pieces = refs[:count]
    own_ref, other_ref = refs[count : count + 2]
    at = count + 2
    head_refs = refs[at : at + nets]
    at += nets
    if with_actions:
        act_ref, act_w_ref = refs[at : at + 2]
        at += 2
    hidden_refs = refs[at : at + nets]
    part_ref, buf, w_buf, sems, w_sems = refs[at + nets :]
    rows = buf.shape[2]
    w_copies = [
        pltpu.make_async_copy(ref, w_buf.at[i], w_sems.at[i])
        for i, ref in enumerate((own_ref, other_ref))
    ]
    copies = [
        pltpu.make_async_copy(pieces[i], buf.at[j, :, pl.ds(start, size), :], sems.at[i])
        for i, (j, start, size) in enumerate(places)
    ]
    row = row_ref[0]
    w_copies[0].start()
    for j in range(row_count):
        for i, (jj, _, _) in enumerate(places):
            if jj == j:
                copies[i].start()
        if j == 0:
            w_copies[1].start()
    for w_copy in w_copies:
        w_copy.wait()
    for j in range(row_count):
        for i, (jj, _, _) in enumerate(places):
            if jj == j:
                copies[i].wait()
        where = jnp.bitwise_xor(row, j)
        for n in range(nets):
            acc = jnp.dot(buf[j, 0], w_buf[0, picks[n]], preferred_element_type=F32)
            acc = acc + jnp.dot(buf[j, 1], w_buf[1, picks[n]], preferred_element_type=F32)
            if with_actions:
                acc = acc + jnp.dot(act_ref[where], act_w_ref[n], preferred_element_type=F32)
            hidden = jnp.maximum(acc, 0.0).astype(BF16)
            hidden_refs[n][where] = hidden
    for j in range(row_count):
        at = 0
        for n in range(nets):
            part = lax.dot_general(
                head_refs[n][...], hidden_refs[n][j], (((1,), (1,)), ((), ())),
                preferred_element_type=F32,
            )
            if with_actions:
                part_ref[n : n + 1, j * rows : (j + 1) * rows] = part[0:1]
            else:
                part_ref[j, at : at + part.shape[0], :] = part
            at += part.shape[0]


def run_nets(row_at, pieces, places, w_own, w_other, heads, rows, row_count, extra, picks):
    nets, depth, units = w_own.shape
    any_spec = pl.BlockSpec(memory_space=pl.ANY)
    vmem = pl.BlockSpec(memory_space=pltpu.VMEM)
    smem = pl.BlockSpec(memory_space=pltpu.SMEM)
    late = [w_own, w_other, *heads, *extra]
    tokens = row_count * rows
    wide = max(units, 128)
    held = 4 * tokens * depth + 4 * nets * depth * wide + 2 * nets * tokens * wide
    outs = pl.pallas_call(
        functools.partial(
            net_kernel, places=places, row_count=row_count, picks=picks,
            with_actions=bool(extra),
        ),
        out_shape=tuple(
            [jax.ShapeDtypeStruct((row_count, rows, units), BF16)] * nets
            + [jax.ShapeDtypeStruct((nets, tokens) if extra else (row_count, 32, rows), F32)]
        ),
        in_specs=[smem] + [any_spec] * (len(pieces) + 2) + [vmem] * (len(late) - 2),
        out_specs=tuple([vmem] * (nets + 1)),
        scratch_shapes=[
            pltpu.VMEM((row_count, 2, rows, depth), BF16),
            pltpu.VMEM((2, nets, depth, units), BF16),
            pltpu.SemaphoreType.DMA((len(pieces),)),
            pltpu.SemaphoreType.DMA((2,)),
        ],
        compiler_params=pltpu.CompilerParams(vmem_limit_bytes=held + 4 * 1024 * 1024),
        cost_estimate=pl.CostEstimate(
            flops=4 * nets * tokens * depth * units,
            bytes_accessed=4 * tokens * depth,
            transcendentals=0,
        ),
    )(row_at.reshape(1), *pieces, *late)
    return outs[:nets], outs[nets]


def split_dot(coeff, hidden):
    high = coeff.astype(BF16)
    low = (coeff - high.astype(F32)).astype(BF16)
    out = jnp.dot(high, hidden, preferred_element_type=F32)
    return out + jnp.dot(low, hidden, preferred_element_type=F32)


def in_parts(coeff, first, last):
    count, cut, _ = first.shape
    size = cut + last.shape[1]
    total = None
    for j in range(count):
        for ref, low, high in ((first, 0, cut), (last, cut, size)):
            term = split_dot(coeff[:, j * size + low : j * size + high], ref[j])
            total = term if total is None else total + term
    return total


def tail_kernel(
    dp_ref, late_ref, pack_ref, known_ref, scale_ref, h0, h1, h2, h2_last, h3, h3_last,
    adv_ref, out_ref, grad_ref, *rest, acts,
):
    sources = (h0, h1, h2, h2_last, h3, h3_last)
    copies = [
        pltpu.make_async_copy(source, held, rest[-1].at[i])
        for i, (source, held) in enumerate(zip(sources, rest[:-1]))
    ]
    for copy in copies:
        copy.start()
    h0, h1, h2, h2_last, h3, h3_last = rest[:-1]
    tokens = late_ref.shape[-1]
    dp = dp_ref[0]
    values = [known_ref[acts + d : acts + d + 1] for d in range(2)]
    advs = [
        jnp.minimum(late_ref[2 * d : 2 * d + 1], late_ref[2 * d + 1 : 2 * d + 2]) - values[d]
        for d in range(2)
    ]
    first, second, adv = late_ref[0:1], late_ref[1:2], advs[0]
    top = functools.reduce(jnp.maximum, [jnp.max(a) for a in advs])
    values = [jnp.where(dp == 0, values[0], values[1]), jnp.where(dp == 0, values[1], values[0])]
    rewards = pack_ref[acts : acts + 1]
    terminal = pack_ref[acts + 1 : acts + 2]
    index = pack_ref[acts + 2 : acts + 3].astype(jnp.int32)
    lanes = 128
    groups = tokens // lanes
    table = jnp.concatenate(
        [v[:, g * lanes : (g + 1) * lanes] for v in values for g in range(groups)], axis=0
    )
    high = jnp.right_shift(index, 7)
    low = jnp.bitwise_and(index, lanes - 1)
    pick_high = (lax.broadcasted_iota(jnp.int32, (table.shape[0], tokens), 0) == high).astype(F32)
    rows = lax.dot_general(
        table, pick_high, (((0,), (0,)), ((), ())), precision=lax.Precision.HIGHEST,
        preferred_element_type=F32,
    )
    pick_low = lax.broadcasted_iota(jnp.int32, (lanes, tokens), 0) == low
    following = jnp.sum(jnp.where(pick_low, rows, 0.0), axis=0, keepdims=True)
    target = rewards + GAMMA * (1.0 - terminal) * following
    weight = jnp.maximum(jnp.exp(adv - top), FLOOR)
    expectile = jnp.where(adv >= 0.0, TAU, 1.0 - TAU)
    scale = scale_ref[...]
    scaled = (pack_ref[0:acts] - known_ref[0:acts]) / scale
    log_prob = -0.5 * jnp.sum(scaled * scaled, axis=0, keepdims=True)
    gap0 = first - target
    gap1 = second - target
    loss0 = jnp.sum(expectile * adv * adv)
    loss1 = jnp.sum(gap0 * gap0 + gap1 * gap1)
    loss2 = -jnp.sum(weight * log_prob)
    adv_ref[...] = adv
    lane = lax.broadcasted_iota(jnp.int32, (1, grad_ref.shape[1]), 1)
    loss = jnp.where(lane == 0, loss0, jnp.where(lane == 1, loss1, jnp.where(lane == 2, loss2, 0.0)))
    high = loss.astype(BF16).astype(F32)
    grad_ref[acts + 3 : acts + 4] = high
    grad_ref[acts + 4 : acts + 5] = loss - high
    for copy in copies:
        copy.wait()
    grad_ref[0:1] = split_dot(2.0 * gap0, h0[...])
    grad_ref[1:2] = split_dot(2.0 * gap1, h1[...])
    grad_ref[2:3] = in_parts(-2.0 * expectile * adv, h2, h2_last)
    grad_ref[3 : 3 + acts] = in_parts(-weight * scaled / scale, h3, h3_last)
    out = grad_ref[...].astype(BF16)
    for i in range(out_ref.shape[0]):
        out_ref[i] = out


def shards(
    states, actions, rewards, terminal, next_index, hidden_weights, action_weights, heads, policy_scale
):
    rows, feats = states.shape
    acts = actions.shape[1]
    _, _, row_units = hidden_weights.shape
    row_count = lax.axis_size("row")
    col_count = lax.axis_size("col")
    dp_count = lax.axis_size("dp")
    dp_at = lax.axis_index("dp")
    row_at = lax.axis_index("row")
    col_at = lax.axis_index("col")
    peers = row_count * col_count
    units = row_units // col_count
    half = feats // 2
    tokens = rows * row_count
    total = tokens * dp_count
    shares = (1, 3, 4, 3, 1) if rows % 192 == 0 else (1, 1)
    sizes = [rows * s // sum(shares) for s in shares]
    starts = [sum(sizes[:c]) for c in range(len(sizes))]

    pack = jnp.concatenate(
        [
            actions.astype(F32).T,
            rewards[None],
            terminal.astype(F32)[None],
            next_index.astype(F32)[None],
        ],
        axis=0,
    )
    pack = spread(pack, ("row",))
    own_actions = pack[:, :acts].transpose(0, 2, 1).astype(BF16)
    pack = pack.transpose(1, 0, 2).reshape(acts + 3, tokens)

    col_bits = bits_of(col_count)[::-1]
    cols = [0]
    for bit in col_bits:
        cols = cols + [c ^ bit for c in cols]
    pair = states.reshape(rows, 2, half).transpose(1, 0, 2)
    pair = jnp.where(dp_at == 0, pair, pair[::-1])
    pieces, places = [], []
    for c, (start, size) in enumerate(zip(starts, sizes)):
        block = pair[:, start : start + size]
        for bit in col_bits:
            got = swap(block, "col", bit)
            block = jnp.concatenate([block, got], axis=2)
        held = {0: block}
        order = bits_of(row_count)
        if c % 2:
            order = order[::-1]
        for bit in order:
            for j, value in list(held.items()):
                held[j ^ bit] = swap(value, "row", bit)
        for j in range(row_count):
            pieces.append(held[j])
            places.append((j, start, size))

    cut = rows * 2 // 3 if rows % 192 == 0 else starts[-1]
    calls = [
        [(p, (j, at, size)) for p, (j, at, size) in zip(pieces, places) if at < cut],
        [(p, (j, at - cut, size)) for p, (j, at, size) in zip(pieces, places) if at >= cut],
    ]
    unit_at = row_at * row_units + col_at * units
    heads_t = lax.dynamic_slice_in_dim(heads.T, unit_at, units, 1)
    act_w = lax.dynamic_slice_in_dim(action_weights, unit_at, units, 2)
    rest = jnp.zeros((7, units), heads.dtype)
    head = [jnp.concatenate([heads_t[n : n + 1], rest], axis=0) for n in range(3)]
    head.append(heads_t[3:])
    exchanged = []
    for first in (0, 2):
        low = 2 - first
        mine = lax.dynamic_slice(hidden_weights, (low, dp_at * half, 0), (2, half, row_units))
        got = []
        for k in cols:
            sent = lax.dynamic_slice_in_dim(mine, jnp.bitwise_xor(col_at, k) * units, units, 2)
            if k == col_count - 1:
                inner = {col_count // 2 - 1, col_count // 2}
                near = [(i, i ^ k) for i in range(col_count) if i in inner]
                far = [(i, i ^ k) for i in range(col_count) if i not in inner]
                near = lax.ppermute(sent, "col", near)
                far = lax.ppermute(sent, "col", far)
                is_near = (col_at == col_count // 2 - 1) | (col_at == col_count // 2)
                got.append(jnp.where(is_near, near, far))
            else:
                got.append(swap(sent, "col", k) if k else sent)
        w_own = jnp.concatenate(got, axis=1)
        exchanged.append((w_own, swap(w_own, "dp", 1)))
    known, hidden_parts = [], []
    for call, size in zip(calls, (cut, rows - cut)):
        some, part = run_nets(
            row_at, [p for p, _ in call], [q for _, q in call], *exchanged[0],
            [head[3], head[2]], size, row_count, (), (1, 0),
        )
        known.append(part)
        hidden_parts.append(some)
    critics, late = run_nets(
        row_at, pieces, places, *exchanged[1], head[:2], rows, row_count,
        (own_actions, act_w), (0, 1),
    )

    group = 32 // col_count
    known = jnp.concatenate(known, axis=2).reshape(peers, group, rows)
    known = lax.all_to_all(known, ("row", "col"), 0, 0, tiled=True)
    known = jnp.sum(known, axis=0)
    at = acts % group
    other = swap(known[at : at + 1], "dp", 1)
    spot = (lax.broadcasted_iota(jnp.int32, known.shape, 0) == at + 1) & (col_at == acts // group)
    known = jnp.where(spot, other, known)
    known = spread(known, ("row", "col"))
    known = known.reshape(row_count, 32, rows).transpose(1, 0, 2).reshape(32, tokens)

    for axis, size in (("col", col_count), ("row", row_count)):
        late = sum((swap(late, axis, k) for k in range(1, size)), late)
    late = jnp.concatenate([late, swap(late, "dp", 1)], axis=0)

    vmem = pl.BlockSpec(memory_space=pltpu.VMEM)
    smem = pl.BlockSpec(memory_space=pltpu.SMEM)
    hidden = [h.reshape(tokens, units) for h in critics]
    hidden += [hidden_parts[i][n] for n in (1, 0) for i in (0, 1)]
    adv, last = pl.pallas_call(
        functools.partial(tail_kernel, acts=acts),
        out_shape=(
            jax.ShapeDtypeStruct((1, tokens), F32),
            jax.ShapeDtypeStruct((dp_count * peers, acts + 5, units), BF16),
        ),
        in_specs=[smem] + [vmem] * 4 + [pl.BlockSpec(memory_space=pl.ANY)] * 6,
        out_specs=(vmem, vmem),
        scratch_shapes=[
            pltpu.VMEM((acts + 5, units), F32),
            *[pltpu.VMEM(h.shape, BF16) for h in hidden],
            pltpu.SemaphoreType.DMA((len(hidden),)),
        ],
        compiler_params=pltpu.CompilerParams(vmem_limit_bytes=24 * 1024 * 1024),
    )(
        dp_at.reshape(1), late, pack, known, policy_scale[:, None],
        *hidden,
    )
    advantage = lax.dynamic_slice_in_dim(adv[0], row_at * rows, rows, 0)
    last = lax.all_to_all(last, ("dp", "row", "col"), 0, 0, tiled=True)
    last = last.reshape(dp_count, peers, acts + 5, units)
    summed = jnp.sum(last.astype(F32), axis=0)
    grads = summed[:, : acts + 3].transpose(1, 0, 2).reshape(acts + 3, peers * units)
    grads = (grads / math.sqrt(total)).T
    losses = (summed[0, acts + 3, :3] + summed[0, acts + 4, :3]) / total
    return advantage, losses, grads


def solution(mesh):
    return jax.shard_map(
        shards,
        mesh=mesh,
        in_specs=(
            P(("dp", "row"), "col"),
            P(("dp", "row"), None),
            P(("dp", "row")),
            P(("dp", "row")),
            P(("dp", "row")),
            P(None, "col", "row"),
            P(),
            P(),
            P(),
        ),
        out_specs=(P(("dp", "row")), P(), P()),
        check_vma=False,
    )
```
